32 devices in a mesh: rep: 4 (over y, x), fsdp: 2 (over core), tp: 4 (over z).
Axes of the slice: x: 2, y: 2, z: 4, core: 2. Of those that a mesh axis runs over, the one named last changes fastest.
Arguments:
- hidden: bfloat16 [128, 3584], P(('rep', 'fsdp')), may hold values from -6 to 6
- head_weight: bfloat16 [3072, 3584], P(('fsdp', 'tp')), may hold values from -0.09375 to 0.09375
- labels: int32 [128], P(('rep', 'fsdp')), may hold values from 0 to 3071
Outputs:
- grad_hidden: bfloat16 [128, 3584], P(('rep', 'fsdp'), 'tp')
- grad_head: float32 [3072, 3584], P(('fsdp', 'tp', 'rep'))
- token_loss: float32 [128], P(('rep', 'fsdp'))
- top_logprob: float32 [128], P(('rep', 'fsdp'))
- grad_norm: float32 [1], replicated
The draws below stay inside these ranges and needn't reach their ends.
Inputs may be any that keep to these rules, and one draw needn't show every extreme that they name: labels[t] is a vocabulary index from 0 to 3071, a few indices being very common.
All inputs are finite; a program needn't handle non-finite values.
Results may differ from the reference program's by a relative error of at most 0.0015.
Values may be sent and summed in bfloat16 or wider, within the bound.
A program may use at most 64 MiB of HBM per device.

```python
import math
import jax
import jax.numpy as jnp
import numpy as np
from jax import lax

D = 3584
VOCAB = 3072
TOKENS = 128


def touch_ends(drawn, key, smallest, top_value):
    extent = drawn.shape
    index_at = [jax.random.randint(jax.random.fold_in(key, axis), (), 0, extent[axis]) for axis in range(len(extent))]
    drawn = drawn.at[tuple(index_at)].set(smallest)
    longest = extent.index(max(extent))
    index_at[longest] = (index_at[longest] + 1) % extent[longest]
    return drawn.at[tuple(index_at)].set(top_value)


def block_levels(rng, dims, pieces, low, largest):
    level, own = 1.0, jax.random.fold_in(rng, 6)
    for position, shards_of in pieces:
        heights = jnp.exp(jax.random.uniform(jax.random.fold_in(own, position), (shards_of,), jnp.float32, low / len(pieces), largest / len(pieces)))
        level = level * jnp.repeat(heights, dims[position] // shards_of).reshape([-1 if axis == position else 1 for axis in range(len(dims))])
    return level


def rank_table(amount, slope):
    portions = [(1 << 20) // math.isqrt(grade ** slope) + 1 for grade in range(1, amount + 1)]
    deviation = 1 + sum(portions) // (1 << 30)
    return np.cumsum(np.array([max(1, weight // deviation) for weight in portions]))


def ranked_ids(key, extent, amount, skew):
    table = rank_table(amount, skew)
    lot = jax.random.randint(jax.random.fold_in(key, 1), extent, 0, int(table[amount - 1]))
    standing = jnp.searchsorted(jnp.asarray(table, jnp.int32), lot, side="right")
    return jax.random.permutation(jax.random.fold_in(key, 2), amount)[standing].astype(jnp.int32)


def noise(key, dims, width, bound, cuts=(), kind=jnp.bfloat16):
    loudness = block_levels(key, dims, cuts, -0.22, 0.18) if cuts else 1.0
    array = jax.random.normal(key, dims, jnp.float32) * width * loudness
    return jnp.minimum(jnp.maximum(array, -bound), bound).astype(kind)


def setup_inputs(seed: int = 0) -> dict:
    splits = jax.random.split(jax.random.key(seed), 4)
    hidden = noise(splits[0], (TOKENS, D), 1.0, 6.0, ((0, 8),))
    head_weight = noise(splits[1], (VOCAB, D), D ** -0.5, 0.09375, ((0, 8),))
    labels = touch_ends(ranked_ids(splits[2], (TOKENS,), VOCAB, 3), jax.random.fold_in(splits[2], 3), 0, VOCAB - 1).astype(jnp.int32)
    return dict(hidden=hidden, head_weight=head_weight, labels=labels)


def reference(hidden, head_weight, labels):
    logits = jnp.dot(hidden, head_weight.T, preferred_element_type=jnp.float32)
    row_max = lax.optimization_barrier(jnp.max(logits, axis=1))
    log_norm = row_max + jnp.log(lax.optimization_barrier(jnp.sum(jnp.exp(logits - row_max[:, None]), axis=1)))
    vocab_ids = lax.broadcasted_iota(jnp.int32, logits.shape, 1)
    chosen = vocab_ids == labels.astype(jnp.int32)[:, None]
    label_logit = lax.optimization_barrier(jnp.sum(jnp.where(chosen, logits, jnp.zeros_like(logits)), axis=1))
    token_loss = log_norm - label_logit
    top_logprob = row_max - log_norm
    probabilities = jnp.exp(logits - log_norm[:, None])
    grad_logits = (probabilities - chosen.astype(jnp.float32)).astype(jnp.bfloat16)
    grad_hidden = jnp.dot(grad_logits, head_weight, preferred_element_type=jnp.float32).astype(jnp.bfloat16)
    grad_head = jnp.dot(grad_logits.T, hidden, preferred_element_type=jnp.float32)
    grad_norm = jnp.sqrt(jnp.sum(grad_head * grad_head)).reshape(1)
    return (grad_hidden, grad_head, token_loss, top_logprob, grad_norm)
```

```python
import functools

import jax
import jax.numpy as jnp
from jax import lax
from jax.experimental import pallas as pl
from jax.experimental.pallas import tpu as pltpu
from jax.sharding import PartitionSpec as P

MESH = pl.DeviceIdType.MESH
LANES = 128


def flipped(values, to_row):
    n = max(values.shape)
    square = (n, n)
    same = lax.broadcasted_iota(jnp.int32, square, 0) == lax.broadcasted_iota(jnp.int32, square, 1)
    spread = jnp.where(same, jnp.broadcast_to(values, square), 0.0)
    return jnp.sum(spread, axis=0 if to_row else 1, keepdims=True)


def kernel(
    R, F, T,
    hidden_hbm, head_hbm, labels_ref,
    gh_ref, grad_head_hbm, loss_ref, top_ref, norm_ref,
    hid, head, labs, logits, stats, gl, gl_send, gl_all,
    part, s1_send, s1_recv, s2_send, s2_recv, gout, nrm1, nrm2,
    in_sem, head_sem, out_sem,
    hs_send, hs_recv, fw_send, fw_recv, ls_send, ls_recv,
    st_send, st_recv, gl_ss, gl_rs, s1_ss, s1_rs, s2_ss, s2_rs,
    n1_ss, n1_rs, n2_ss, n2_rs,
):
    r, f, t = lax.axis_index("rep"), lax.axis_index("fsdp"), lax.axis_index("tp")
    n = hidden_hbm.shape[0]
    vocab, width = head.shape
    own_vocab = vocab // R
    cols = width // T
    group = F * n

    def at(k, a, b):
        return (lax.rem(r + k + R, R), lax.rem(f + a + F, F), lax.rem(t + b + T, T))

    sent = []

    def send(src, dst, ss, rs, where):
        copy = pltpu.make_async_remote_copy(
            src_ref=src, dst_ref=dst, send_sem=ss, recv_sem=rs, device_id=at(*where), device_id_type=MESH
        )
        copy.start()
        sent.append(copy)

    def arrived(dst, ss, rs, where):
        pltpu.make_async_remote_copy(
            src_ref=dst, dst_ref=dst, send_sem=ss, recv_sem=rs, device_id=at(*where), device_id_type=MESH
        ).wait_recv()

    own = pltpu.make_async_copy(hidden_hbm, hid.at[0, 0], in_sem)
    own.start()
    blocks = vocab // LANES
    loads = []
    for i in range(blocks):
        rows = pl.ds(i * LANES, LANES)
        loads.append(pltpu.make_async_copy(head_hbm.at[rows], head.at[rows], head_sem.at[i]))
        loads[-1].start()

    peers = [(k, 0, 0) for k in range(1, R)]
    mates = [(0, a, b) for a in range(F) for b in range(T) if a or b]
    barrier = pltpu.get_barrier_semaphore()
    for where in peers + mates:
        pl.semaphore_signal(barrier, inc=1, device_id=at(*where), device_id_type=MESH)
    pl.semaphore_wait(barrier, len(peers) + len(mates))

    own.wait()
    for a in range(1, F):
        send(labels_ref, labs.at[a - 1], ls_send.at[a - 1], ls_recv.at[a - 1], (0, a, 0))
        send(hid.at[0, 0], hid.at[0, a], hs_send.at[0, a - 1], hs_recv.at[0, a - 1], (0, a, 0))
    for k in range(1, R):
        send(hid.at[0, 0], hid.at[k, 0], fw_send.at[k - 1], fw_recv.at[k - 1], (k, 0, 0))

    for a in range(1, F):
        arrived(labs.at[a - 1], ls_send.at[a - 1], ls_recv.at[a - 1], (0, a, 0))
        arrived(hid.at[0, a], hs_send.at[0, a - 1], hs_recv.at[0, a - 1], (0, a, 0))
    tokens = hid[0].reshape(group, width)
    for i in range(blocks):
        loads[i].wait()
        logits[:, i * LANES : (i + 1) * LANES] = lax.dot_general(
            tokens, head[i * LANES : (i + 1) * LANES, :], (((1,), (1,)), ((), ())),
            preferred_element_type=jnp.float32,
        )

    label_rows = [labels_ref[...]] + [labs[a - 1] for a in range(1, F)]
    label_cols = [flipped(row.astype(jnp.float32), False).astype(jnp.int32) for row in label_rows]
    labels = jnp.concatenate(label_cols, axis=0) if F > 1 else label_cols[0]
    vocab_start = (f * T + t) * vocab
    scores = logits[...]
    chosen = lax.broadcasted_iota(jnp.int32, scores.shape, 1) == labels - vocab_start
    local_max = jnp.max(scores, axis=1, keepdims=True)
    local_sum = jnp.sum(jnp.exp(scores - local_max), axis=1, keepdims=True)
    label_part = jnp.sum(jnp.where(chosen, scores, 0.0), axis=1, keepdims=True)
    lane = lax.broadcasted_iota(jnp.int32, (group, LANES), 1)
    stats[0] = jnp.where(lane == 0, local_max, jnp.where(lane == 1, local_sum, label_part))
    for k, a, b in mates:
        slot = a * T + b
        send(stats.at[0], stats.at[slot], st_send.at[slot - 1], st_recv.at[slot - 1], (0, a, b))

    for k in range(1, R):
        arrived(hid.at[k, 0], fw_send.at[k - 1], fw_recv.at[k - 1], (k, 0, 0))
        for a in range(1, F):
            send(hid.at[k, 0], hid.at[k, a], hs_send.at[k, a - 1], hs_recv.at[k, a - 1], (0, a, 0))

    for k, a, b in mates:
        slot = a * T + b
        arrived(stats.at[slot], st_send.at[slot - 1], st_recv.at[slot - 1], (0, a, b))

    def from_mate(slot):
        a = slot // T
        if a == 0:
            return stats[slot]
        pieces = [stats[slot, ((c - a) % F) * n : ((c - a) % F + 1) * n, :] for c in range(F)]
        return jnp.concatenate(pieces, axis=0)

    tables = [from_mate(slot) for slot in range(F * T)]
    row_max = functools.reduce(jnp.maximum, [table[:, 0:1] for table in tables])
    row_sum = sum(table[:, 1:2] * jnp.exp(table[:, 0:1] - row_max) for table in tables)
    label_logit = sum(table[:, 2:3] for table in tables)
    log_norm = row_max + jnp.log(row_sum)
    grad = jnp.exp(logits[...] - log_norm) - chosen.astype(jnp.float32)
    for k in range(R):
        gl_send[k] = grad[:, k * own_vocab : (k + 1) * own_vocab].astype(jnp.bfloat16)
    gl[...] = grad.astype(jnp.bfloat16)
    for k in range(1, R):
        send(
            gl_send.at[lax.rem(r + k, R)], gl_all.at[k], gl_ss.at[k - 1], gl_rs.at[k - 1], (k, 0, 0)
        )
    gl_all[0] = gl_send[r]

    order = list(range(1, T)) + [0]
    for b in order:
        start = pl.multiple_of(lax.rem(t + b, T) * cols, cols)
        piece = jnp.dot(gl[...], head[:, pl.ds(start, cols)], preferred_element_type=jnp.float32)
        part[b] = piece[:n]
        for a in range(1, F):
            s1_send[a - 1, b] = piece[a * n : (a + 1) * n]
            send(
                s1_send.at[a - 1, b], s1_recv.at[a - 1, b], s1_ss.at[a - 1, b], s1_rs.at[a - 1, b],
                (0, -a, 0),
            )
    for b in order:
        total = part[b]
        for a in range(1, F):
            arrived(s1_recv.at[a - 1, b], s1_ss.at[a - 1, b], s1_rs.at[a - 1, b], (0, a, 0))
            total = total + s1_recv[a - 1, b]
        if b:
            s2_send[b - 1] = total
            send(s2_send.at[b - 1], s2_recv.at[b - 1], s2_ss.at[b - 1], s2_rs.at[b - 1], (0, 0, b))
        else:
            part[0] = total

    own_loss = flipped((log_norm - label_logit)[:n], True)
    loss_ref[...] = own_loss
    top_ref[...] = flipped((row_max - log_norm)[:n], True)

    for k in range(1, R):
        arrived(gl_all.at[k], gl_ss.at[k - 1], gl_rs.at[k - 1], (k, 0, 0))
        for a in range(1, F):
            arrived(hid.at[k, a], hs_send.at[k, a - 1], hs_recv.at[k, a - 1], (0, a, 0))
    all_gl = gl_all[...].reshape(R * group, own_vocab)
    squares = jnp.zeros((8, cols), jnp.float32)
    outs = []
    for b in range(T):
        span = slice(b * cols, (b + 1) * cols)
        piece = lax.dot_general(
            all_gl, hid[:, :, :, span].reshape(R * group, cols), (((0,), (0,)), ((), ())),
            preferred_element_type=jnp.float32,
        )
        gout[:, span] = piece
        outs.append(pltpu.make_async_copy(gout.at[:, span], grad_head_hbm.at[:, span], out_sem.at[b]))
        outs[-1].start()
        squares = squares + jnp.sum((piece * piece).reshape(own_vocab // 8, 8, cols), axis=0)
    nrm1[0] = sum(squares[:, i * LANES : (i + 1) * LANES] for i in range(cols // LANES))
    for k in range(1, R):
        send(nrm1.at[0], nrm1.at[k], n1_ss.at[k - 1], n1_rs.at[k - 1], (k, 0, 0))
    for k in range(1, R):
        arrived(nrm1.at[k], n1_ss.at[k - 1], n1_rs.at[k - 1], (k, 0, 0))
    nrm2[0] = jnp.sum(nrm1[...], axis=0)
    for k, a, b in mates:
        slot = a * T + b
        send(nrm2.at[0], nrm2.at[slot], n2_ss.at[slot - 1], n2_rs.at[slot - 1], (0, a, b))

    total = part[0]
    for b in range(1, T):
        arrived(s2_recv.at[b - 1], s2_ss.at[b - 1], s2_rs.at[b - 1], (0, 0, b))
        total = total + s2_recv[b - 1]
    gh_ref[...] = total.astype(jnp.bfloat16)

    for k, a, b in mates:
        slot = a * T + b
        arrived(nrm2.at[slot], n2_ss.at[slot - 1], n2_rs.at[slot - 1], (0, a, b))
    lanes = jnp.sum(jnp.sum(nrm2[...], axis=0), axis=0, keepdims=True)
    norm_ref[...] = jnp.sqrt(jnp.sum(lanes, axis=1, keepdims=True))

    for copy in sent:
        copy.wait_send()
    for copy in outs:
        copy.wait()


def local(R, F, T, hidden, head_weight, labels):
    n, width = hidden.shape
    vocab = head_weight.shape[0]
    own_vocab = vocab // R
    cols = width // T
    group = F * n
    f32, bf16 = jnp.float32, jnp.bfloat16
    dma = pltpu.SemaphoreType.DMA
    vmem = pl.BlockSpec(memory_space=pltpu.VMEM)
    hbm = pl.BlockSpec(memory_space=pl.ANY)
    FM = max(F - 1, 1)
    slots = F * T
    scratch = [
        pltpu.VMEM((R, F, n, width), bf16),
        pltpu.VMEM((vocab, width), bf16),
        pltpu.VMEM((FM, 1, n), jnp.int32),
        pltpu.VMEM((group, vocab), f32),
        pltpu.VMEM((slots, group, LANES), f32),
        pltpu.VMEM((group, vocab), bf16),
        pltpu.VMEM((R, group, own_vocab), bf16),
        pltpu.VMEM((R, group, own_vocab), bf16),
        pltpu.VMEM((T, n, cols), f32),
        pltpu.VMEM((FM, T, n, cols), f32),
        pltpu.VMEM((FM, T, n, cols), f32),
        pltpu.VMEM((T - 1, n, cols), f32),
        pltpu.VMEM((T - 1, n, cols), f32),
        pltpu.VMEM((own_vocab, width), f32),
        pltpu.VMEM((R, 8, LANES), f32),
        pltpu.VMEM((slots, 8, LANES), f32),
        dma(()), dma((vocab // LANES,)), dma((T,)),
        dma((R, FM)), dma((R, FM)), dma((R - 1,)), dma((R - 1,)), dma((FM,)), dma((FM,)),
        dma((slots - 1,)), dma((slots - 1,)), dma((R - 1,)), dma((R - 1,)),
        dma((FM, T)), dma((FM, T)), dma((T - 1,)), dma((T - 1,)),
        dma((R - 1,)), dma((R - 1,)), dma((slots - 1,)), dma((slots - 1,)),
    ]
    grad_hidden, grad_head, loss, top, norm = pl.pallas_call(
        functools.partial(kernel, R, F, T),
        out_shape=(
            jax.ShapeDtypeStruct((n, cols), bf16),
            jax.ShapeDtypeStruct((own_vocab, width), f32),
            jax.ShapeDtypeStruct((1, n), f32),
            jax.ShapeDtypeStruct((1, n), f32),
            jax.ShapeDtypeStruct((1, 1), f32),
        ),
        in_specs=[hbm, hbm, vmem],
        out_specs=(vmem, hbm, vmem, vmem, vmem),
        scratch_shapes=scratch,
        compiler_params=pltpu.CompilerParams(
            collective_id=0, has_side_effects=True, vmem_limit_bytes=60 * 1024 * 1024
        ),
    )(hidden, head_weight, labels.reshape(1, n))
    return (grad_hidden, grad_head, loss.reshape(n), top.reshape(n), norm.reshape(1))


def solution(mesh):
    in_specs = (P(("rep", "fsdp"), None), P(("fsdp", "tp"), None), P(("rep", "fsdp")))
    out_specs = (
        P(("rep", "fsdp"), "tp"),
        P(("fsdp", "tp", "rep"), None),
        P(("rep", "fsdp")),
        P(("rep", "fsdp")),
        P(),
    )
    body = functools.partial(local, mesh.shape["rep"], mesh.shape["fsdp"], mesh.shape["tp"])
    return jax.shard_map(body, mesh=mesh, in_specs=in_specs, out_specs=out_specs, check_vma=False)
```

```python
import functools

import jax
import jax.numpy as jnp
from jax import lax
from jax.experimental import pallas as pl
from jax.experimental.pallas import tpu as pltpu
from jax.sharding import PartitionSpec as P

MESH = pl.DeviceIdType.MESH
LANES = 128


def flipped(values, to_row):
    n = max(values.shape)
    square = (n, n)
    same = lax.broadcasted_iota(jnp.int32, square, 0) == lax.broadcasted_iota(jnp.int32, square, 1)
    spread = jnp.where(same, jnp.broadcast_to(values, square), 0.0)
    return jnp.sum(spread, axis=0 if to_row else 1, keepdims=True)


def kernel(
    R, F, T,
    hidden_hbm, head_hbm, labels_ref,
    gh_ref, gout, loss_ref, top_ref, norm_ref,
    hid, head, labs, logits, stats_send, stats, gl, gl_send, gl_all,
    part, s1_send, s1_recv, s2_send, s2_recv, nrm1, nrm2,
    in_sem, head_sem,
    hs_send, hs_recv, fw_send, fw_recv, ls_send, ls_recv,
    st_send, st_recv, gl_ss, gl_rs, s1_ss, s1_rs, s2_ss, s2_rs,
    n1_ss, n1_rs, n2_ss, n2_rs,
):
    r, f, t = lax.axis_index("rep"), lax.axis_index("fsdp"), lax.axis_index("tp")
    n = hidden_hbm.shape[0]
    vocab, width = head.shape
    own_vocab = vocab // R
    cols = width // T
    group = F * n

    def at(k, a, b):
        return (lax.rem(r + k + R, R), lax.rem(f + a + F, F), lax.rem(t + b + T, T))

    sent = []

    def send(src, dst, ss, rs, where):
        copy = pltpu.make_async_remote_copy(
            src_ref=src, dst_ref=dst, send_sem=ss, recv_sem=rs, device_id=at(*where), device_id_type=MESH
        )
        copy.start()
        sent.append(copy)

    def arrived(dst, ss, rs, where):
        pltpu.make_async_remote_copy(
            src_ref=dst, dst_ref=dst, send_sem=ss, recv_sem=rs, device_id=at(*where), device_id_type=MESH
        ).wait_recv()

    own = pltpu.make_async_copy(hidden_hbm, hid.at[0, 0], in_sem)
    own.start()
    blocks = vocab // LANES
    loads = []
    for i in range(blocks):
        rows = pl.ds(i * LANES, LANES)
        loads.append(pltpu.make_async_copy(head_hbm.at[rows], head.at[rows], head_sem.at[i]))
        loads[-1].start()

    peers = [(k, 0, 0) for k in range(1, R)]
    mates = [(0, a, b) for a in range(F) for b in range(T) if a or b]
    barrier = pltpu.get_barrier_semaphore()
    for where in peers + mates:
        pl.semaphore_signal(barrier, inc=1, device_id=at(*where), device_id_type=MESH)
    pl.semaphore_wait(barrier, len(peers) + len(mates))

    own.wait()
    for a in range(1, F):
        send(labels_ref, labs.at[a - 1], ls_send.at[a - 1], ls_recv.at[a - 1], (0, a, 0))
        send(hid.at[0, 0], hid.at[0, a], hs_send.at[0, a - 1], hs_recv.at[0, a - 1], (0, a, 0))
    for k in range(1, R):
        send(hid.at[0, 0], hid.at[k, 0], fw_send.at[k - 1], fw_recv.at[k - 1], (k, 0, 0))

    for a in range(1, F):
        arrived(labs.at[a - 1], ls_send.at[a - 1], ls_recv.at[a - 1], (0, a, 0))
        arrived(hid.at[0, a], hs_send.at[0, a - 1], hs_recv.at[0, a - 1], (0, a, 0))
    tokens = hid[0].reshape(group, width)
    for i in range(blocks):
        loads[i].wait()
        logits[:, i * LANES : (i + 1) * LANES] = lax.dot_general(
            tokens, head[i * LANES : (i + 1) * LANES, :], (((1,), (1,)), ((), ())),
            preferred_element_type=jnp.float32,
        )

    label_rows = [labels_ref[...]] + [labs[a - 1] for a in range(1, F)]
    label_cols = [flipped(row.astype(jnp.float32), False).astype(jnp.int32) for row in label_rows]
    labels = jnp.concatenate(label_cols, axis=0) if F > 1 else label_cols[0]
    vocab_start = (f * T + t) * vocab
    scores = logits[...]
    chosen = lax.broadcasted_iota(jnp.int32, scores.shape, 1) == labels - vocab_start
    local_max = jnp.max(scores, axis=1, keepdims=True)
    local_sum = jnp.sum(jnp.exp(scores - local_max), axis=1, keepdims=True)
    label_part = jnp.sum(jnp.where(chosen, scores, 0.0), axis=1, keepdims=True)
    lane = lax.broadcasted_iota(jnp.int32, (group, LANES), 1)
    packed = jnp.where(lane == 0, local_max, jnp.where(lane == 1, local_sum, label_part))
    for a in range(F):
        turned = packed if a == 0 else jnp.concatenate([packed[(F - a) * n :], packed[: (F - a) * n]], axis=0)
        stats_send[a] = turned.T[:8]
    for k, a, b in mates:
        slot = a * T + b
        send(stats_send.at[a], stats.at[slot], st_send.at[slot - 1], st_recv.at[slot - 1], (0, a, b))
    stats[0] = stats_send[0]

    for k in range(1, R):
        arrived(hid.at[k, 0], fw_send.at[k - 1], fw_recv.at[k - 1], (k, 0, 0))
        for a in range(1, F):
            send(hid.at[k, 0], hid.at[k, a], hs_send.at[k, a - 1], hs_recv.at[k, a - 1], (0, a, 0))

    for k, a, b in mates:
        slot = a * T + b
        arrived(stats.at[slot], st_send.at[slot - 1], st_recv.at[slot - 1], (0, a, b))
    tables = [stats[slot] for slot in range(F * T)]
    row_max = functools.reduce(jnp.maximum, [table[0:1] for table in tables])
    row_sum = sum(table[1:2] * jnp.exp(table[0:1] - row_max) for table in tables)
    label_logit = sum(table[2:3] for table in tables)
    log_row = row_max + jnp.log(row_sum)
    log_norm = flipped(log_row, False)
    grad = jnp.exp(logits[...] - log_norm) - chosen.astype(jnp.float32)
    for k in range(R):
        gl_send[k] = grad[:, k * own_vocab : (k + 1) * own_vocab].astype(jnp.bfloat16)
    gl[...] = grad.astype(jnp.bfloat16)
    for k in range(1, R):
        send(
            gl_send.at[lax.rem(r + k, R)], gl_all.at[k], gl_ss.at[k - 1], gl_rs.at[k - 1], (k, 0, 0)
        )
    gl_all[0] = gl_send[r]

    order = list(range(1, T)) + [0]
    for b in order:
        start = pl.multiple_of(lax.rem(t + b, T) * cols, cols)
        piece = jnp.dot(gl[...], head[:, pl.ds(start, cols)], preferred_element_type=jnp.float32)
        part[b] = piece[:n]
        for a in range(1, F):
            s1_send[a - 1, b] = piece[a * n : (a + 1) * n]
            send(
                s1_send.at[a - 1, b], s1_recv.at[a - 1, b], s1_ss.at[a - 1, b], s1_rs.at[a - 1, b],
                (0, -a, 0),
            )
    for b in order:
        total = part[b]
        for a in range(1, F):
            arrived(s1_recv.at[a - 1, b], s1_ss.at[a - 1, b], s1_rs.at[a - 1, b], (0, a, 0))
            total = total + s1_recv[a - 1, b]
        if b:
            s2_send[b - 1] = total
            send(s2_send.at[b - 1], s2_recv.at[b - 1], s2_ss.at[b - 1], s2_rs.at[b - 1], (0, 0, b))
        else:
            part[0] = total

    loss_ref[...] = (log_row - label_logit)[:, :n]
    top_ref[...] = (row_max - log_row)[:, :n]

    for k in range(1, R):
        arrived(gl_all.at[k], gl_ss.at[k - 1], gl_rs.at[k - 1], (k, 0, 0))
        for a in range(1, F):
            arrived(hid.at[k, a], hs_send.at[k, a - 1], hs_recv.at[k, a - 1], (0, a, 0))
    all_gl = gl_all[...].reshape(R * group, own_vocab)
    squares = jnp.zeros((8, cols), jnp.float32)
    for b in range(T):
        span = slice(b * cols, (b + 1) * cols)
        piece = lax.dot_general(
            all_gl, hid[:, :, :, span].reshape(R * group, cols), (((0,), (0,)), ((), ())),
            preferred_element_type=jnp.float32,
        )
        gout[:, span] = piece
        squares = squares + jnp.sum((piece * piece).reshape(own_vocab // 8, 8, cols), axis=0)
    nrm1[0] = sum(squares[:, i * LANES : (i + 1) * LANES] for i in range(cols // LANES))
    for k in range(1, R):
        send(nrm1.at[0], nrm1.at[k], n1_ss.at[k - 1], n1_rs.at[k - 1], (k, 0, 0))
    for k in range(1, R):
        arrived(nrm1.at[k], n1_ss.at[k - 1], n1_rs.at[k - 1], (k, 0, 0))
    nrm2[0] = jnp.sum(nrm1[...], axis=0)
    for k, a, b in mates:
        slot = a * T + b
        send(nrm2.at[0], nrm2.at[slot], n2_ss.at[slot - 1], n2_rs.at[slot - 1], (0, a, b))

    total = part[0]
    for b in range(1, T):
        arrived(s2_recv.at[b - 1], s2_ss.at[b - 1], s2_rs.at[b - 1], (0, 0, b))
        total = total + s2_recv[b - 1]
    gh_ref[...] = total.astype(jnp.bfloat16)

    for k, a, b in mates:
        slot = a * T + b
        arrived(nrm2.at[slot], n2_ss.at[slot - 1], n2_rs.at[slot - 1], (0, a, b))
    lanes = jnp.sum(jnp.sum(nrm2[...], axis=0), axis=0, keepdims=True)
    norm_ref[...] = jnp.sqrt(jnp.sum(lanes, axis=1, keepdims=True))

    for copy in sent:
        copy.wait_send()


def store(*refs):
    count = (len(refs) - 1) // 2
    sources, targets, sems = refs[:count], refs[count : 2 * count], refs[-1]
    copies = [
        pltpu.make_async_copy(sources[i], targets[i], sems.at[i]) for i in range(count - 1)
    ]
    for copy in copies:
        copy.start()
    targets[-1][...] = sources[-1][...]
    for copy in copies:
        copy.wait()


def local(R, F, T, hidden, head_weight, labels):
    n, width = hidden.shape
    vocab = head_weight.shape[0]
    own_vocab = vocab // R
    cols = width // T
    group = F * n
    f32, bf16 = jnp.float32, jnp.bfloat16
    dma = pltpu.SemaphoreType.DMA
    vmem = pl.BlockSpec(memory_space=pltpu.VMEM)
    anywhere = pl.BlockSpec(memory_space=pl.ANY)
    hbm = pl.BlockSpec(memory_space=pltpu.HBM)
    FM = max(F - 1, 1)
    slots = F * T
    scratch = [
        pltpu.VMEM((R, F, n, width), bf16),
        pltpu.VMEM((vocab, width), bf16),
        pltpu.VMEM((FM, 1, n), jnp.int32),
        pltpu.VMEM((group, vocab), f32),
        pltpu.VMEM((F, 8, group), f32),
        pltpu.VMEM((slots, 8, group), f32),
        pltpu.VMEM((group, vocab), bf16),
        pltpu.VMEM((R, group, own_vocab), bf16),
        pltpu.VMEM((R, group, own_vocab), bf16),
        pltpu.VMEM((T, n, cols), f32),
        pltpu.VMEM((FM, T, n, cols), f32),
        pltpu.VMEM((FM, T, n, cols), f32),
        pltpu.VMEM((T - 1, n, cols), f32),
        pltpu.VMEM((T - 1, n, cols), f32),
        pltpu.VMEM((R, 8, LANES), f32),
        pltpu.VMEM((slots, 8, LANES), f32),
        dma(()), dma((vocab // LANES,)),
        dma((R, FM)), dma((R, FM)), dma((R - 1,)), dma((R - 1,)), dma((FM,)), dma((FM,)),
        dma((slots - 1,)), dma((slots - 1,)), dma((R - 1,)), dma((R - 1,)),
        dma((FM, T)), dma((FM, T)), dma((T - 1,)), dma((T - 1,)),
        dma((R - 1,)), dma((R - 1,)), dma((slots - 1,)), dma((slots - 1,)),
    ]
    shapes = [((n, cols), bf16), ((own_vocab, width), f32), ((1, n), f32), ((1, n), f32), ((1, 1), f32)]
    grant = 67_043_328 - 4 * own_vocab * width - 2 * n * cols - 32 * 1024
    held = pl.pallas_call(
        functools.partial(kernel, R, F, T),
        out_shape=tuple(pltpu.VMEM(shape, dtype) for shape, dtype in shapes),
        in_specs=[hbm, hbm, vmem],
        out_specs=(vmem,) * 5,
        scratch_shapes=scratch,
        compiler_params=pltpu.CompilerParams(
            collective_id=0, has_side_effects=True, vmem_limit_bytes=grant
        ),
    )(hidden, head_weight, labels.reshape(1, n))
    grad_hidden, grad_head, loss, top, norm = pl.pallas_call(
        store,
        out_shape=tuple(jax.ShapeDtypeStruct(shape, dtype) for shape, dtype in shapes),
        in_specs=[anywhere] * 4 + [vmem],
        out_specs=(hbm,) * 4 + (vmem,),
        scratch_shapes=[dma((4,))],
        compiler_params=pltpu.CompilerParams(vmem_limit_bytes=1024 * 1024),
    )(*held)
    return (grad_hidden, grad_head, loss.reshape(n), top.reshape(n), norm.reshape(1))


def solution(mesh):
    in_specs = (P(("rep", "fsdp"), None), P(("fsdp", "tp"), None), P(("rep", "fsdp")))
    out_specs = (
        P(("rep", "fsdp"), "tp"),
        P(("fsdp", "tp", "rep"), None),
        P(("rep", "fsdp")),
        P(("rep", "fsdp")),
        P(),
    )
    body = functools.partial(local, mesh.shape["rep"], mesh.shape["fsdp"], mesh.shape["tp"])
    return jax.shard_map(body, mesh=mesh, in_specs=in_specs, out_specs=out_specs, check_vma=False)
```

```python
import functools

import jax
import jax.numpy as jnp
from jax import lax
from jax.experimental import pallas as pl
from jax.experimental.pallas import tpu as pltpu
from jax.sharding import PartitionSpec as P

MESH = pl.DeviceIdType.MESH
LANES = 128


def flipped(values, to_row):
    n = max(values.shape)
    square = (n, n)
    same = lax.broadcasted_iota(jnp.int32, square, 0) == lax.broadcasted_iota(jnp.int32, square, 1)
    spread = jnp.where(same, jnp.broadcast_to(values, square), 0.0)
    return jnp.sum(spread, axis=0 if to_row else 1, keepdims=True)


def kernel(
    R, F, T,
    hidden_hbm, head_hbm, labels_ref,
    gh_ref, gout, loss_ref, top_ref, norm_ref,
    hid, head, labs, logits, stats_send, stats, gl, gl_send, gl_all,
    part, s1_send, s1_recv, s2_send, s2_recv, nrm1, nrm2,
    in_sem, head_sem,
    hs_send, hs_recv, fw_send, fw_recv, ls_send, ls_recv,
    st_send, st_recv, gl_ss, gl_rs, s1_ss, s1_rs, s2_ss, s2_rs,
    n1_ss, n1_rs, n2_ss, n2_rs,
):
    r, f, t = lax.axis_index("rep"), lax.axis_index("fsdp"), lax.axis_index("tp")
    n = hidden_hbm.shape[0]
    vocab, width = head.shape
    own_vocab = vocab // R
    cols = width // T
    group = F * n

    def at(k, a, b):
        if R == 4 and k:
            rep = (r, r + 1 - 2 * lax.rem(r, 2), lax.rem(r + 2, 4), 3 - r)[k]
        else:
            rep = lax.rem(r + k, R)
        return (rep, lax.rem(f + a + F, F), lax.rem(t + b + T, T))

    sent = []

    def send(src, dst, ss, rs, where):
        copy = pltpu.make_async_remote_copy(
            src_ref=src, dst_ref=dst, send_sem=ss, recv_sem=rs, device_id=at(*where), device_id_type=MESH
        )
        copy.start()
        sent.append(copy)

    def arrived(dst, ss, rs, where):
        pltpu.make_async_remote_copy(
            src_ref=dst, dst_ref=dst, send_sem=ss, recv_sem=rs, device_id=at(*where), device_id_type=MESH
        ).wait_recv()

    own = pltpu.make_async_copy(hidden_hbm, hid.at[0, 0], in_sem)
    own.start()
    blocks = vocab // LANES
    loads = []
    for i in range(blocks):
        rows = pl.ds(i * LANES, LANES)
        loads.append(pltpu.make_async_copy(head_hbm.at[rows], head.at[rows], head_sem.at[i]))
        loads[-1].start()

    peers = [(k, 0, 0) for k in range(1, R)]
    mates = [(0, a, b) for a in range(F) for b in range(T) if a or b]
    barrier = pltpu.get_barrier_semaphore()
    for where in peers + mates:
        pl.semaphore_signal(barrier, inc=1, device_id=at(*where), device_id_type=MESH)
    pl.semaphore_wait(barrier, len(peers) + len(mates))

    own.wait()
    for a in range(1, F):
        send(labels_ref, labs.at[a - 1], ls_send.at[a - 1], ls_recv.at[a - 1], (0, a, 0))
        send(hid.at[0, 0], hid.at[0, a], hs_send.at[0, a - 1], hs_recv.at[0, a - 1], (0, a, 0))
    halves = [pl.ds(0, width // 2), pl.ds(width // 2, width // 2)]

    def pass_on(source, k, h, to):
        send(
            hid.at[source, 0, :, halves[h]], hid.at[k, 0, :, halves[h]],
            fw_send.at[k - 1, h], fw_recv.at[k - 1, h], (to, 0, 0),
        )

    def landed(k, h):
        arrived(hid.at[k, 0, :, halves[h]], fw_send.at[k - 1, h], fw_recv.at[k - 1, h], (k, 0, 0))

    relays = [(1, 0, 2), (2, 1, 1)] if R == 4 else []
    direct = 3 if relays else R
    for k in range(1, direct):
        for h in (0, 1) if k == 1 else (1, 0):
            pass_on(0, k, h, k)

    for a in range(1, F):
        arrived(labs.at[a - 1], ls_send.at[a - 1], ls_recv.at[a - 1], (0, a, 0))
        arrived(hid.at[0, a], hs_send.at[0, a - 1], hs_recv.at[0, a - 1], (0, a, 0))
    tokens = hid[0].reshape(group, width)
    for i in range(blocks):
        loads[i].wait()
        logits[:, i * LANES : (i + 1) * LANES] = lax.dot_general(
            tokens, head[i * LANES : (i + 1) * LANES, :], (((1,), (1,)), ((), ())),
            preferred_element_type=jnp.float32,
        )

    label_rows = [labels_ref[...]] + [labs[a - 1] for a in range(1, F)]
    label_cols = [flipped(row.astype(jnp.float32), False).astype(jnp.int32) for row in label_rows]
    labels = jnp.concatenate(label_cols, axis=0) if F > 1 else label_cols[0]
    vocab_start = (f * T + t) * vocab
    scores = logits[...]
    chosen = lax.broadcasted_iota(jnp.int32, scores.shape, 1) == labels - vocab_start
    local_max = jnp.max(scores, axis=1, keepdims=True)
    local_sum = jnp.sum(jnp.exp(scores - local_max), axis=1, keepdims=True)
    label_part = jnp.sum(jnp.where(chosen, scores, 0.0), axis=1, keepdims=True)
    lane = lax.broadcasted_iota(jnp.int32, (group, LANES), 1)
    packed = jnp.where(lane == 0, local_max, jnp.where(lane == 1, local_sum, label_part))
    for a in range(F):
        turned = packed if a == 0 else jnp.concatenate([packed[(F - a) * n :], packed[: (F - a) * n]], axis=0)
        stats_send[a] = turned.T[:8]
    for k, a, b in mates:
        slot = a * T + b
        send(stats_send.at[a], stats.at[slot], st_send.at[slot - 1], st_recv.at[slot - 1], (0, a, b))
    stats[0] = stats_send[0]

    for k, h, to in relays:
        landed(k, h)
        pass_on(k, 3, h, to)

    for k, a, b in mates:
        slot = a * T + b
        arrived(stats.at[slot], st_send.at[slot - 1], st_recv.at[slot - 1], (0, a, b))
    tables = [stats[slot] for slot in range(F * T)]
    row_max = functools.reduce(jnp.maximum, [table[0:1] for table in tables])
    row_sum = sum(table[1:2] * jnp.exp(table[0:1] - row_max) for table in tables)
    label_logit = sum(table[2:3] for table in tables)
    log_row = row_max + jnp.log(row_sum)
    log_norm = flipped(log_row, False)
    grad = jnp.exp(logits[...] - log_norm) - chosen.astype(jnp.float32)
    for k in range(R):
        gl_send[k] = grad[:, k * own_vocab : (k + 1) * own_vocab].astype(jnp.bfloat16)
    gl[...] = grad.astype(jnp.bfloat16)
    for k in range(1, R):
        send(
            gl_send.at[at(k, 0, 0)[0]], gl_all.at[k], gl_ss.at[k - 1], gl_rs.at[k - 1], (k, 0, 0)
        )
    gl_all[0] = gl_send[r]

    order = list(range(1, T)) + [0]
    for b in order:
        start = pl.multiple_of(lax.rem(t + b, T) * cols, cols)
        piece = jnp.dot(gl[...], head[:, pl.ds(start, cols)], preferred_element_type=jnp.float32)
        part[b] = piece[:n]
        for a in range(1, F):
            s1_send[a - 1, b] = piece[a * n : (a + 1) * n]
            send(
                s1_send.at[a - 1, b], s1_recv.at[a - 1, b], s1_ss.at[a - 1, b], s1_rs.at[a - 1, b],
                (0, -a, 0),
            )
    for b in order:
        total = part[b]
        for a in range(1, F):
            arrived(s1_recv.at[a - 1, b], s1_ss.at[a - 1, b], s1_rs.at[a - 1, b], (0, a, 0))
            total = total + s1_recv[a - 1, b]
        if b:
            s2_send[b - 1] = total
            send(s2_send.at[b - 1], s2_recv.at[b - 1], s2_ss.at[b - 1], s2_rs.at[b - 1], (0, 0, b))
        else:
            part[0] = total

    for k in range(1, R):
        for h in range(2):
            if all((k, h) != relay[:2] for relay in relays):
                landed(k, h)
        for a in range(1, F):
            send(hid.at[k, 0], hid.at[k, a], hs_send.at[k, a - 1], hs_recv.at[k, a - 1], (0, a, 0))

    loss_ref[...] = (log_row - label_logit)[:, :n]
    top_ref[...] = (row_max - log_row)[:, :n]

    for k in range(1, R):
        arrived(gl_all.at[k], gl_ss.at[k - 1], gl_rs.at[k - 1], (k, 0, 0))
        for a in range(1, F):
            arrived(hid.at[k, a], hs_send.at[k, a - 1], hs_recv.at[k, a - 1], (0, a, 0))
    all_gl = gl_all[...].reshape(R * group, own_vocab)
    squares = jnp.zeros((8, cols), jnp.float32)
    for b in range(T):
        span = slice(b * cols, (b + 1) * cols)
        piece = lax.dot_general(
            all_gl, hid[:, :, :, span].reshape(R * group, cols), (((0,), (0,)), ((), ())),
            preferred_element_type=jnp.float32,
        )
        gout[:, span] = piece
        squares = squares + jnp.sum((piece * piece).reshape(own_vocab // 8, 8, cols), axis=0)
    nrm1[0] = sum(squares[:, i * LANES : (i + 1) * LANES] for i in range(cols // LANES))
    for k in range(1, R):
        send(nrm1.at[0], nrm1.at[k], n1_ss.at[k - 1], n1_rs.at[k - 1], (k, 0, 0))
    for k in range(1, R):
        arrived(nrm1.at[k], n1_ss.at[k - 1], n1_rs.at[k - 1], (k, 0, 0))
    nrm2[0] = jnp.sum(nrm1[...], axis=0)
    for k, a, b in mates:
        slot = a * T + b
        send(nrm2.at[0], nrm2.at[slot], n2_ss.at[slot - 1], n2_rs.at[slot - 1], (0, a, b))

    total = part[0]
    for b in range(1, T):
        arrived(s2_recv.at[b - 1], s2_ss.at[b - 1], s2_rs.at[b - 1], (0, 0, b))
        total = total + s2_recv[b - 1]
    gh_ref[...] = total.astype(jnp.bfloat16)

    for k, a, b in mates:
        slot = a * T + b
        arrived(nrm2.at[slot], n2_ss.at[slot - 1], n2_rs.at[slot - 1], (0, a, b))
    lanes = jnp.sum(jnp.sum(nrm2[...], axis=0), axis=0, keepdims=True)
    norm_ref[...] = jnp.sqrt(jnp.sum(lanes, axis=1, keepdims=True))

    for copy in sent:
        copy.wait_send()


def store(*refs):
    count = (len(refs) - 1) // 2
    sources, targets, sems = refs[:count], refs[count : 2 * count], refs[-1]
    copies = [
        pltpu.make_async_copy(sources[i], targets[i], sems.at[i]) for i in range(count - 1)
    ]
    for copy in copies:
        copy.start()
    targets[-1][...] = sources[-1][...]
    for copy in copies:
        copy.wait()


def local(R, F, T, hidden, head_weight, labels):
    n, width = hidden.shape
    vocab = head_weight.shape[0]
    own_vocab = vocab // R
    cols = width // T
    group = F * n
    f32, bf16 = jnp.float32, jnp.bfloat16
    dma = pltpu.SemaphoreType.DMA
    vmem = pl.BlockSpec(memory_space=pltpu.VMEM)
    anywhere = pl.BlockSpec(memory_space=pl.ANY)
    hbm = pl.BlockSpec(memory_space=pltpu.HBM)
    FM = max(F - 1, 1)
    slots = F * T
    scratch = [
        pltpu.VMEM((R, F, n, width), bf16),
        pltpu.VMEM((vocab, width), bf16),
        pltpu.VMEM((FM, 1, n), jnp.int32),
        pltpu.VMEM((group, vocab), f32),
        pltpu.VMEM((F, 8, group), f32),
        pltpu.VMEM((slots, 8, group), f32),
        pltpu.VMEM((group, vocab), bf16),
        pltpu.VMEM((R, group, own_vocab), bf16),
        pltpu.VMEM((R, group, own_vocab), bf16),
        pltpu.VMEM((T, n, cols), f32),
        pltpu.VMEM((FM, T, n, cols), f32),
        pltpu.VMEM((FM, T, n, cols), f32),
        pltpu.VMEM((T - 1, n, cols), f32),
        pltpu.VMEM((T - 1, n, cols), f32),
        pltpu.VMEM((R, 8, LANES), f32),
        pltpu.VMEM((slots, 8, LANES), f32),
        dma(()), dma((vocab // LANES,)),
        dma((R, FM)), dma((R, FM)), dma((R - 1, 2)), dma((R - 1, 2)), dma((FM,)), dma((FM,)),
        dma((slots - 1,)), dma((slots - 1,)), dma((R - 1,)), dma((R - 1,)),
        dma((FM, T)), dma((FM, T)), dma((T - 1,)), dma((T - 1,)),
        dma((R - 1,)), dma((R - 1,)), dma((slots - 1,)), dma((slots - 1,)),
    ]
    shapes = [((n, cols), bf16), ((own_vocab, width), f32), ((1, n), f32), ((1, n), f32), ((1, 1), f32)]
    grant = 67_043_328 - 4 * own_vocab * width - 2 * n * cols - 32 * 1024
    held = pl.pallas_call(
        functools.partial(kernel, R, F, T),
        out_shape=tuple(pltpu.VMEM(shape, dtype) for shape, dtype in shapes),
        in_specs=[hbm, hbm, vmem],
        out_specs=(vmem,) * 5,
        scratch_shapes=scratch,
        compiler_params=pltpu.CompilerParams(
            collective_id=0, has_side_effects=True, vmem_limit_bytes=grant
        ),
    )(hidden, head_weight, labels.reshape(1, n))
    grad_hidden, grad_head, loss, top, norm = pl.pallas_call(
        store,
        out_shape=tuple(jax.ShapeDtypeStruct(shape, dtype) for shape, dtype in shapes),
        in_specs=[anywhere] * 4 + [vmem],
        out_specs=(hbm,) * 4 + (vmem,),
        scratch_shapes=[dma((4,))],
        compiler_params=pltpu.CompilerParams(vmem_limit_bytes=1024 * 1024),
    )(*held)
    return (grad_hidden, grad_head, loss.reshape(n), top.reshape(n), norm.reshape(1))


def solution(mesh):
    in_specs = (P(("rep", "fsdp"), None), P(("fsdp", "tp"), None), P(("rep", "fsdp")))
    out_specs = (
        P(("rep", "fsdp"), "tp"),
        P(("fsdp", "tp", "rep"), None),
        P(("rep", "fsdp")),
        P(("rep", "fsdp")),
        P(),
    )
    body = functools.partial(local, mesh.shape["rep"], mesh.shape["fsdp"], mesh.shape["tp"])
    return jax.shard_map(body, mesh=mesh, in_specs=in_specs, out_specs=out_specs, check_vma=False)
```

```python
import functools

import jax
import jax.numpy as jnp
from jax import lax
from jax.experimental import pallas as pl
from jax.experimental.pallas import tpu as pltpu
from jax.sharding import PartitionSpec as P

MESH = pl.DeviceIdType.MESH
LANES = 128


def flipped(values, to_row):
    n = max(values.shape)
    square = (n, n)
    same = lax.broadcasted_iota(jnp.int32, square, 0) == lax.broadcasted_iota(jnp.int32, square, 1)
    spread = jnp.where(same, jnp.broadcast_to(values, square), 0.0)
    return jnp.sum(spread, axis=0 if to_row else 1, keepdims=True)


def kernel(
    R, F, T,
    hidden_hbm, head_hbm, labels_ref,
    gh_ref, gout, loss_ref, top_ref, norm_ref,
    hid, head, labs, logits, stats_send, stats, gl, gl_send, gl_all,
    part, s1_send, s1_recv, s2_send, s2_recv, nrm1, nrm2,
    in_sem, head_sem,
    hs_send, hs_recv, fw_send, fw_recv, ls_send, ls_recv,
    st_send, st_recv, gl_ss, gl_rs, s1_ss, s1_rs, s2_ss, s2_rs,
    n1_ss, n1_rs, n2_ss, n2_rs,
):
    r, f, t = lax.axis_index("rep"), lax.axis_index("fsdp"), lax.axis_index("tp")
    n = hidden_hbm.shape[0]
    vocab, width = head.shape
    own_vocab = vocab // R
    cols = width // T
    group = F * n

    def at(k, a, b):
        return (lax.rem(r + k + R, R), lax.rem(f + a + F, F), lax.rem(t + b + T, T))

    sent = []

    def send(src, dst, ss, rs, where):
        copy = pltpu.make_async_remote_copy(
            src_ref=src, dst_ref=dst, send_sem=ss, recv_sem=rs, device_id=at(*where), device_id_type=MESH
        )
        copy.start()
        sent.append(copy)

    def arrived(dst, ss, rs, where):
        pltpu.make_async_remote_copy(
            src_ref=dst, dst_ref=dst, send_sem=ss, recv_sem=rs, device_id=at(*where), device_id_type=MESH
        ).wait_recv()

    own = pltpu.make_async_copy(hidden_hbm, hid.at[0, 0], in_sem)
    own.start()
    blocks = vocab // LANES
    loads = []
    for i in range(blocks):
        rows = pl.ds(i * LANES, LANES)
        loads.append(pltpu.make_async_copy(head_hbm.at[rows], head.at[rows], head_sem.at[i]))
        loads[-1].start()

    def score_block(i, first, last):
        rows = slice(first * n, last * n)
        block = lax.dot_general(
            head[i * LANES : (i + 1) * LANES, :], hid[0, first:last].reshape((last - first) * n, width),
            (((1,), (1,)), ((), ())), preferred_element_type=jnp.float32,
        )
        logits[rows, i * LANES : (i + 1) * LANES] = block.T

    peers = [(k, 0, 0) for k in range(1, R)]
    mates = [(0, a, b) for a in range(F) for b in range(T) if a or b]
    barrier = pltpu.get_barrier_semaphore()
    for where in peers + mates:
        pl.semaphore_signal(barrier, inc=1, device_id=at(*where), device_id_type=MESH)
    pl.semaphore_wait(barrier, len(peers) + len(mates))

    own.wait()
    for a in range(1, F):
        send(labels_ref, labs.at[a - 1], ls_send.at[a - 1], ls_recv.at[a - 1], (0, a, 0))
        send(hid.at[0, 0], hid.at[0, a], hs_send.at[0, a - 1], hs_recv.at[0, a - 1], (0, a, 0))
    for k in range(1, R):
        send(hid.at[0, 0], hid.at[k, 0], fw_send.at[k - 1], fw_recv.at[k - 1], (k, 0, 0))

    for a in range(1, F):
        arrived(labs.at[a - 1], ls_send.at[a - 1], ls_recv.at[a - 1], (0, a, 0))
        arrived(hid.at[0, a], hs_send.at[0, a - 1], hs_recv.at[0, a - 1], (0, a, 0))
    for i in range(blocks):
        loads[i].wait()
        score_block(i, 0, F)

    label_rows = [labels_ref[...]] + [labs[a - 1] for a in range(1, F)]
    label_cols = [flipped(row.astype(jnp.float32), False).astype(jnp.int32) for row in label_rows]
    labels = jnp.concatenate(label_cols, axis=0) if F > 1 else label_cols[0]
    vocab_start = (f * T + t) * vocab
    scores = logits[...]
    chosen = lax.broadcasted_iota(jnp.int32, scores.shape, 1) == labels - vocab_start
    local_max = jnp.max(scores, axis=1, keepdims=True)
    local_sum = jnp.sum(jnp.exp(scores - local_max), axis=1, keepdims=True)
    label_part = jnp.sum(jnp.where(chosen, scores, 0.0), axis=1, keepdims=True)
    lane = lax.broadcasted_iota(jnp.int32, (group, LANES), 1)
    packed = jnp.where(lane == 0, local_max, jnp.where(lane == 1, local_sum, label_part))
    for a in range(F):
        turned = packed if a == 0 else jnp.concatenate([packed[(F - a) * n :], packed[: (F - a) * n]], axis=0)
        stats_send[a] = turned.T[:8]
    for k, a, b in mates:
        slot = a * T + b
        send(stats_send.at[a], stats.at[slot], st_send.at[slot - 1], st_recv.at[slot - 1], (0, a, b))
    stats[0] = stats_send[0]

    for k in range(1, R):
        arrived(hid.at[k, 0], fw_send.at[k - 1], fw_recv.at[k - 1], (k, 0, 0))
        for a in range(1, F):
            send(hid.at[k, 0], hid.at[k, a], hs_send.at[k, a - 1], hs_recv.at[k, a - 1], (0, a, 0))

    for k, a, b in mates:
        slot = a * T + b
        arrived(stats.at[slot], st_send.at[slot - 1], st_recv.at[slot - 1], (0, a, b))
    tables = [stats[slot] for slot in range(F * T)]
    row_max = functools.reduce(jnp.maximum, [table[0:1] for table in tables])
    row_sum = sum(table[1:2] * jnp.exp(table[0:1] - row_max) for table in tables)
    label_logit = sum(table[2:3] for table in tables)
    log_row = row_max + jnp.log(row_sum)
    log_norm = flipped(log_row, False)
    grad = jnp.exp(logits[...] - log_norm) - chosen.astype(jnp.float32)
    for k in range(R):
        gl_send[k] = grad[:, k * own_vocab : (k + 1) * own_vocab].astype(jnp.bfloat16)
    gl[...] = grad.astype(jnp.bfloat16)
    for k in range(1, R):
        send(
            gl_send.at[lax.rem(r + k, R)], gl_all.at[k], gl_ss.at[k - 1], gl_rs.at[k - 1], (k, 0, 0)
        )
    gl_all[0] = gl_send[r]

    order = list(range(1, T)) + [0]
    for b in order:
        start = pl.multiple_of(lax.rem(t + b, T) * cols, cols)
        piece = jnp.dot(gl[...], head[:, pl.ds(start, cols)], preferred_element_type=jnp.float32)
        part[b] = piece[:n]
        for a in range(1, F):
            s1_send[a - 1, b] = piece[a * n : (a + 1) * n]
            send(
                s1_send.at[a - 1, b], s1_recv.at[a - 1, b], s1_ss.at[a - 1, b], s1_rs.at[a - 1, b],
                (0, -a, 0),
            )
    for b in order:
        total = part[b]
        for a in range(1, F):
            arrived(s1_recv.at[a - 1, b], s1_ss.at[a - 1, b], s1_rs.at[a - 1, b], (0, a, 0))
            total = total + s1_recv[a - 1, b]
        if b:
            s2_send[b - 1] = total
            send(s2_send.at[b - 1], s2_recv.at[b - 1], s2_ss.at[b - 1], s2_rs.at[b - 1], (0, 0, b))
        else:
            part[0] = total

    loss_ref[...] = (log_row - label_logit)[:, :n]
    top_ref[...] = (row_max - log_row)[:, :n]

    for k in range(1, R):
        arrived(gl_all.at[k], gl_ss.at[k - 1], gl_rs.at[k - 1], (k, 0, 0))
        for a in range(1, F):
            arrived(hid.at[k, a], hs_send.at[k, a - 1], hs_recv.at[k, a - 1], (0, a, 0))
    all_gl = gl_all[...].reshape(R * group, own_vocab)
    squares = jnp.zeros((8, cols), jnp.float32)
    for b in range(T):
        span = slice(b * cols, (b + 1) * cols)
        piece = lax.dot_general(
            all_gl, hid[:, :, :, span].reshape(R * group, cols), (((0,), (0,)), ((), ())),
            preferred_element_type=jnp.float32,
        )
        gout[:, span] = piece
        squares = squares + jnp.sum((piece * piece).reshape(own_vocab // 8, 8, cols), axis=0)
    lanes = sum(squares[:, i * LANES : (i + 1) * LANES] for i in range(cols // LANES))
    nrm1[0] = jnp.sum(lanes, axis=0, keepdims=True)
    for k in range(1, R):
        send(nrm1.at[0], nrm1.at[k], n1_ss.at[k - 1], n1_rs.at[k - 1], (k, 0, 0))
    for k in range(1, R):
        arrived(nrm1.at[k], n1_ss.at[k - 1], n1_rs.at[k - 1], (k, 0, 0))
    nrm2[0] = jnp.sum(nrm1[...], axis=0)
    for k, a, b in mates:
        slot = a * T + b
        send(nrm2.at[0], nrm2.at[slot], n2_ss.at[slot - 1], n2_rs.at[slot - 1], (0, a, b))

    total = part[0]
    for b in range(1, T):
        arrived(s2_recv.at[b - 1], s2_ss.at[b - 1], s2_rs.at[b - 1], (0, 0, b))
        total = total + s2_recv[b - 1]
    gh_ref[...] = total.astype(jnp.bfloat16)

    for k, a, b in mates:
        slot = a * T + b
        arrived(nrm2.at[slot], n2_ss.at[slot - 1], n2_rs.at[slot - 1], (0, a, b))
    lanes = jnp.sum(nrm2[...], axis=0)
    norm_ref[...] = jnp.sqrt(jnp.sum(lanes, axis=1, keepdims=True))

    for copy in sent:
        copy.wait_send()


def store(*refs):
    count = (len(refs) - 1) // 2
    sources, targets, sems = refs[:count], refs[count : 2 * count], refs[-1]
    copies = [
        pltpu.make_async_copy(sources[i], targets[i], sems.at[i]) for i in range(count - 1)
    ]
    for copy in copies:
        copy.start()
    targets[-1][...] = sources[-1][...]
    for copy in copies:
        copy.wait()


def local(R, F, T, hidden, head_weight, labels):
    n, width = hidden.shape
    vocab = head_weight.shape[0]
    own_vocab = vocab // R
    cols = width // T
    group = F * n
    f32, bf16 = jnp.float32, jnp.bfloat16
    dma = pltpu.SemaphoreType.DMA
    vmem = pl.BlockSpec(memory_space=pltpu.VMEM)
    anywhere = pl.BlockSpec(memory_space=pl.ANY)
    hbm = pl.BlockSpec(memory_space=pltpu.HBM)
    FM = max(F - 1, 1)
    slots = F * T
    scratch = [
        pltpu.VMEM((R, F, n, width), bf16),
        pltpu.VMEM((vocab, width), bf16),
        pltpu.VMEM((FM, 1, n), jnp.int32),
        pltpu.VMEM((group, vocab), f32),
        pltpu.VMEM((F, 8, group), f32),
        pltpu.VMEM((slots, 8, group), f32),
        pltpu.VMEM((group, vocab), bf16),
        pltpu.VMEM((R, group, own_vocab), bf16),
        pltpu.VMEM((R, group, own_vocab), bf16),
        pltpu.VMEM((T, n, cols), f32),
        pltpu.VMEM((FM, T, n, cols), f32),
        pltpu.VMEM((FM, T, n, cols), f32),
        pltpu.VMEM((T - 1, n, cols), f32),
        pltpu.VMEM((T - 1, n, cols), f32),
        pltpu.VMEM((R, 1, LANES), f32),
        pltpu.VMEM((slots, 1, LANES), f32),
        dma(()), dma((vocab // LANES,)),
        dma((R, FM)), dma((R, FM)), dma((R - 1,)), dma((R - 1,)), dma((FM,)), dma((FM,)),
        dma((slots - 1,)), dma((slots - 1,)), dma((R - 1,)), dma((R - 1,)),
        dma((FM, T)), dma((FM, T)), dma((T - 1,)), dma((T - 1,)),
        dma((R - 1,)), dma((R - 1,)), dma((slots - 1,)), dma((slots - 1,)),
    ]
    shapes = [((n, cols), bf16), ((own_vocab, width), f32), ((1, n), f32), ((1, n), f32), ((1, 1), f32)]
    grant = 67_043_328 - 4 * own_vocab * width - 2 * n * cols - 32 * 1024
    held = pl.pallas_call(
        functools.partial(kernel, R, F, T),
        out_shape=tuple(pltpu.VMEM(shape, dtype) for shape, dtype in shapes),
        in_specs=[hbm, hbm, vmem],
        out_specs=(vmem,) * 5,
        scratch_shapes=scratch,
        compiler_params=pltpu.CompilerParams(
            collective_id=0, has_side_effects=True, vmem_limit_bytes=grant
        ),
    )(hidden, head_weight, labels.reshape(1, n))
    grad_hidden, grad_head, loss, top, norm = pl.pallas_call(
        store,
        out_shape=tuple(jax.ShapeDtypeStruct(shape, dtype) for shape, dtype in shapes),
        in_specs=[anywhere] * 4 + [vmem],
        out_specs=(hbm,) * 4 + (vmem,),
        scratch_shapes=[dma((4,))],
        compiler_params=pltpu.CompilerParams(vmem_limit_bytes=1024 * 1024),
    )(*held)
    return (grad_hidden, grad_head, loss.reshape(n), top.reshape(n), norm.reshape(1))


def solution(mesh):
    in_specs = (P(("rep", "fsdp"), None), P(("fsdp", "tp"), None), P(("rep", "fsdp")))
    out_specs = (
        P(("rep", "fsdp"), "tp"),
        P(("fsdp", "tp", "rep"), None),
        P(("rep", "fsdp")),
        P(("rep", "fsdp")),
        P(),
    )
    body = functools.partial(local, mesh.shape["rep"], mesh.shape["fsdp"], mesh.shape["tp"])
    return jax.shard_map(body, mesh=mesh, in_specs=in_specs, out_specs=out_specs, check_vma=False)
```
